32 devices in a mesh: groups: 2 (over x), hst: 8 (over z, y), head: 2 (over core).
Axes of the slice: x: 2, y: 2, z: 4, core: 2. Of those that a mesh axis runs over, the one named last changes fastest.
Arguments:
- ctx_query: bfloat16 [3072, 64, 128], P(('groups', 'hst'), 'head'), parts along dimension 0, may hold values from -8 to 8
- ctx_key: bfloat16 [3072, 64, 128], P(('groups', 'hst'), 'head'), parts along dimension 0, may hold values from -8 to 8
- ctx_value: bfloat16 [3072, 64, 128], P(('groups', 'hst'), 'head'), parts along dimension 0, may hold values from -6 to 6
- valid: int32 [16], P(('groups', 'hst')), parts along dimension 0, may hold values from 128 to 192
- tail_query: bfloat16 [128, 64, 128], P(('groups', 'hst'), 'head'), parts along dimension 0, may hold values from -8 to 8
- tail_position: int32 [128], P(('groups', 'hst')), parts along dimension 0, may hold values from 1 to 1536
Outputs:
- ctx_out: bfloat16 [3072, 64, 128], P(('groups', 'hst'), 'head'), parts along dimension 0
- tail_out: bfloat16 [128, 64, 128], P(('groups', 'hst'), 'head'), parts along dimension 0
The draws below stay inside these ranges and needn't reach their ends.
There are 2 independent parts, one for each index of `groups`. The reference program is written for one: setup_inputs(seed, part) draws one part's arguments, and reference() takes and returns one part's arrays. A program takes and returns all parts, laid end to end along the dimension named above; each array names one. Nothing has to cross between parts.
All inputs are finite; a program needn't handle non-finite values.
Results may differ from the reference program's by a relative error of at most 0.0043.
Values may be sent and summed in bfloat16 or wider, within the bound.
No kernel may reach another device: no remote copies, remote signals or barrier semaphores. Data moves between devices by JAX's collectives and lax.ppermute only.
A program may use at most 128 MiB of HBM per device.

```python
import jax
import jax.numpy as jnp
from jax import lax

HEADS = 64
HD = 128
BLOCK = 192
ANCHOR = 128
ROWS = 64
CONTEXT = 1536
N_HST = 8


def draw_ctx_key(key, part):
    base = jnp.clip(jax.random.normal(jax.random.fold_in(key, 202), (CONTEXT, HEADS, HD), jnp.float32), -4.0, 4.0)
    return base.astype(jnp.bfloat16)


def draw_ctx_query(key, part):
    base = jnp.clip(jax.random.normal(jax.random.fold_in(key, 303), (CONTEXT, HEADS, HD), jnp.float32), -4.0, 4.0)
    return base.astype(jnp.bfloat16)


def draw_tail_query(key, part):
    base = jnp.clip(jax.random.normal(jax.random.fold_in(key, 404), (ROWS, HEADS, HD), jnp.float32), -4.0, 4.0)
    return base.astype(jnp.bfloat16)


def plant(result, stream_key, least, high):
    spot = [jax.random.randint(jax.random.fold_in(stream_key, axis), (), 0, length) for axis, length in enumerate(result.shape)]
    longest = result.shape.index(max(result.shape))
    next_to = spot[:longest] + [(spot[longest] + 1) % result.shape[longest]] + spot[longest + 1:]
    return result.at[tuple(spot)].set(least).at[tuple(next_to)].set(high)


def block_scale(own_key, dims, shards, low, top_value):
    def one(position, parts):
        heights = jax.random.uniform(jax.random.fold_in(jax.random.fold_in(own_key, 6), position), (parts,), jnp.float32, low / len(shards), top_value / len(shards))
        return jnp.repeat(jnp.exp(heights), dims[position] // parts).reshape((-1,) + (1,) * (len(dims) - position - 1))

    gain = one(*shards[0])
    for cut in shards[1:]:
        gain = gain * one(*cut)
    return gain


def bell_draw(own_key, dims, deviation, limit, cuts=(), kind=jnp.bfloat16):
    values = deviation * jax.random.normal(own_key, dims, jnp.float32)
    if cuts:
        values = values * block_scale(own_key, dims, cuts, -0.22, 0.18)
    return jnp.clip(values, -limit, limit).astype(kind)


def setup_inputs(seed: int = 0, part: int = 0) -> dict:
    seeds = jax.random.split(jax.random.key(seed), 7)
    own_keys = jax.random.split(jax.random.fold_in(seeds[6], part), 7)
    return {
        "ctx_query": draw_ctx_query(jax.random.fold_in(jax.random.fold_in(seeds[6], part), 71), part),
        "ctx_key": draw_ctx_key(jax.random.fold_in(jax.random.fold_in(seeds[6], part), 71), part),
        "ctx_value": bell_draw(own_keys[2], (CONTEXT, HEADS, HD), 1.0, 6.0, ((0, 8), (1, 2))),
        "valid": plant(jax.random.randint(own_keys[3], (N_HST,), ANCHOR, BLOCK + 1), jax.random.fold_in(own_keys[3], 1), ANCHOR, BLOCK).astype(jnp.int32),
        "tail_query": draw_tail_query(jax.random.fold_in(jax.random.fold_in(seeds[6], part), 71), part),
        "tail_position": plant(jax.random.randint(own_keys[5], (ROWS,), 1, CONTEXT + 1), jax.random.fold_in(own_keys[5], 1), 1, CONTEXT).astype(jnp.int32),
    }


def first_phase(host, query, key, value, count, anchor_key, anchor_value):
    keys = jnp.concatenate([anchor_key, key], 0).astype(jnp.float32)
    values = jnp.concatenate([anchor_value, value], 0).astype(jnp.float32)
    rows = jnp.arange(BLOCK)[:, None]
    cols = jnp.arange(BLOCK)[None, :]
    own_mask = (cols <= rows) & (cols < count)
    anchor_mask = jnp.broadcast_to(host != 0, (BLOCK, ANCHOR))
    mask = jnp.concatenate([anchor_mask, own_mask], 1)
    scores = jnp.einsum('qhd,khd->hqk', query.astype(jnp.float32), keys) / jnp.sqrt(jnp.float32(HD))
    scores = jnp.where(mask[None], scores, jnp.float32(-1e+30))
    peak = lax.optimization_barrier(jnp.max(scores, axis=-1, keepdims=True))
    weights = jnp.where(mask[None], jnp.exp(scores - peak), jnp.float32(0.0))
    total = lax.optimization_barrier(jnp.sum(weights, axis=-1))
    rounded = weights.astype(jnp.bfloat16).astype(jnp.float32)
    summed = jnp.einsum('hqk,khd->qhd', rounded, values)
    return (summed / jnp.transpose(total)[:, :, None]).astype(jnp.bfloat16)

def reference(ctx_query, ctx_key, ctx_value, valid, tail_query, tail_position):
    anchor_key = ctx_key[:ANCHOR]
    anchor_value = ctx_value[:ANCHOR]
    shaped = (HEADS, HD)
    query_blocks = ctx_query.reshape((N_HST, BLOCK) + shaped)
    key_blocks = ctx_key.reshape((N_HST, BLOCK) + shaped)
    value_blocks = ctx_value.reshape((N_HST, BLOCK) + shaped)

    def one_block(items):
        host, query, key, value, count = items
        return first_phase(host, query, key, value, count, anchor_key, anchor_value)
    hosts = jnp.arange(N_HST).astype(jnp.int32)
    ctx_out = lax.map(one_block, (hosts, query_blocks, key_blocks, value_blocks, valid))
    ctx_out = ctx_out.reshape((N_HST * BLOCK,) + shaped)
    starts = (jnp.cumsum(valid) - valid).astype(jnp.int32)
    slots = jnp.arange(BLOCK).astype(jnp.int32)
    positions = (starts[:, None] + slots[None, :]).reshape(-1)
    live = (slots[None, :] < valid[:, None]).reshape(-1)
    mask = live[None, :] & (positions[None, :] < tail_position[:, None])
    scores = jnp.einsum('rhd,khd->hrk', tail_query.astype(jnp.float32), ctx_key.astype(jnp.float32)) / jnp.sqrt(jnp.float32(HD))
    scores = jnp.where(mask[None], scores, jnp.float32(-1e+30))
    peak = lax.optimization_barrier(jnp.max(scores, axis=-1, keepdims=True))
    weights = jnp.where(mask[None], jnp.exp(scores - peak), jnp.float32(0.0))
    total = lax.optimization_barrier(jnp.sum(weights, axis=-1))
    summed = jnp.einsum('hrk,khd->rhd', weights, ctx_value.astype(jnp.float32), precision=lax.Precision.HIGHEST)
    tail_out = (summed / jnp.transpose(total)[:, :, None]).astype(jnp.bfloat16)
    return (ctx_out, tail_out)
```

```python
import functools
import math

import jax
import jax.numpy as jnp
from jax import lax
from jax.experimental import pallas as pl
from jax.experimental.pallas import tpu as pltpu
from jax.sharding import PartitionSpec as P

ANCHOR = 128
GROUP = 8
NEG = -1e30
F32 = jnp.float32
BF16 = jnp.bfloat16
ANY = pl.BlockSpec(memory_space=pl.ANY)
SMEM = pl.BlockSpec(memory_space=pltpu.SMEM)


def dot(a, b, dims):
    return lax.dot_general(a, b, (dims, ((), ())), preferred_element_type=F32)


def pack_kernel(n, valid, position, query, out):
    rows, heads, width = query.shape
    row = lax.broadcasted_iota(jnp.int32, (rows, width), 0)
    lane = lax.broadcasted_iota(jnp.int32, (rows, width), 1)
    slab = jnp.where(lane == 2, valid[0], 0)
    for r in range(rows):
        high = lax.shift_right_logical(position[r], 6)
        low = jnp.bitwise_and(position[r], 63)
        slab = jnp.where((row == r) & (lane == 0), high, slab)
        slab = jnp.where((row == r) & (lane == 1), low, slab)
    slab = slab.astype(F32).astype(BF16)
    for i in range(n):
        out[i, :rows] = query[...]
        out[i, rows, :rows] = slab
        out[i, rows, rows:] = jnp.zeros((heads - rows, width), BF16)


def pack(n, valid, position, query):
    rows, heads, width = query.shape
    return pl.pallas_call(
        functools.partial(pack_kernel, n),
        out_shape=jax.ShapeDtypeStruct((n, rows + 1, heads, width), BF16),
        in_specs=[SMEM, SMEM, pl.BlockSpec(memory_space=pltpu.VMEM)],
        out_specs=pl.BlockSpec(memory_space=pltpu.VMEM),
        name="pack",
    )(valid, position, query)


def part_kernel(rows, scale, valid, query, meta, key, value, out, stats, qs, ks, vs, ms):
    step = pl.program_id(0)
    n = query.shape[0]
    block, group, width = key.shape
    total = n * rows
    me = lax.axis_index("hst")
    qs[...] = query[:, :rows].astype(F32).reshape(total * group, width)
    ks[...] = key[...].astype(F32).reshape(block * group, width)
    vs[...] = value[...].astype(F32).reshape(block * group, width)
    for i in range(n):
        ms[i * rows : (i + 1) * rows] = meta[i, 0].astype(F32)[:rows]
    info = ms[...]
    position = info[:, 0:1] * 64.0 + info[:, 1:2]
    row = lax.broadcasted_iota(jnp.int32, (total, 1), 0)
    ahead = (row < me * rows) & (lax.rem(row, rows) == 0)
    start = jnp.sum(jnp.where(ahead, info[:, 2:3], 0.0), axis=0, keepdims=True)
    slot = lax.broadcasted_iota(jnp.int32, (total, block), 1)
    place = slot.astype(F32) + start
    seen = (place < position) & (slot < valid[0])
    lane = lax.broadcasted_iota(jnp.int32, (total, width), 1)

    @pl.when(step == 0)
    def _():
        stats[...] = jnp.full((total, width), NEG, F32)

    known = stats[...]
    for h in range(group):
        q = qs[pl.ds(h, total, stride=group), :].astype(BF16)
        k = ks[pl.ds(h, block, stride=group), :].astype(BF16)
        v = vs[pl.ds(h, block, stride=group), :].astype(BF16)
        s = jnp.where(seen, dot(q, k, ((1,), (1,))) * scale, NEG)
        peak = jnp.max(s, axis=1, keepdims=True)
        w = jnp.where(seen, jnp.exp(s - peak), 0.0)
        weight = jnp.sum(w, axis=1, keepdims=True)
        w_high = w.astype(BF16)
        w_low = (w - w_high.astype(F32)).astype(BF16)
        o = dot(w_high, v, ((1,), (0,))) + dot(w_low, v, ((1,), (0,)))
        empty = weight == 0.0
        divisor = jnp.where(empty, 1.0, weight)
        o = (o / divisor).astype(BF16)
        lse = jnp.where(empty, NEG, peak + jnp.log(divisor))
        known = jnp.where(lane == step * group + h, lse, known)
        for i in range(n):
            out[i, step * group + h] = o[i * rows : (i + 1) * rows]
    stats[...] = known

    @pl.when(step == pl.num_programs(0) - 1)
    def _():
        at = pl.num_programs(0) * group
        left = stats[...]
        for piece in range(3):
            term = left.astype(BF16)
            left = left - term.astype(F32)
            for i in range(n):
                out[i, at + piece] = term[i * rows : (i + 1) * rows]


def part(valid, far, key, value, scale):
    n, rows, heads, width = far.shape
    rows -= 1
    block = key.shape[0]
    groups = heads // GROUP
    side = pl.BlockSpec((block, GROUP, width), lambda g: (0, g, 0))
    return pl.pallas_call(
        functools.partial(part_kernel, rows, scale),
        grid=(groups,),
        out_shape=jax.ShapeDtypeStruct((n, heads + 3, rows, width), BF16),
        in_specs=[
            SMEM,
            pl.BlockSpec((n, rows + 1, GROUP, width), lambda g: (0, 0, g, 0)),
            pl.BlockSpec((n, 1, GROUP, width), lambda g: (0, rows, 0, 0)),
            side,
            side,
        ],
        out_specs=pl.BlockSpec((n, heads + 3, rows, width), lambda g: (0, 0, 0, 0)),
        scratch_shapes=[
            pltpu.VMEM((n * rows, width), F32),
            pltpu.VMEM((n * rows * GROUP, width), F32),
            pltpu.VMEM((block * GROUP, width), F32),
            pltpu.VMEM((block * GROUP, width), F32),
            pltpu.VMEM((n * rows, width), F32),
        ],
        name="part",
    )(valid, far, far, key, value)


def merge_kernel(rows, heads, parts, out, shares, sums):
    n = parts.shape[0]
    lses = []
    for i in range(n):
        pieces = [parts[i, heads + p].astype(F32) for p in range(3)]
        lses.append(pieces[0] + pieces[1] + pieces[2])
    peak = functools.reduce(jnp.maximum, lses)
    weights = [jnp.exp(lse - peak) for lse in lses]
    total = functools.reduce(jnp.add, weights)
    for i in range(n):
        shares[i] = weights[i] / total
    for h in range(heads):
        acc = None
        for i in range(n):
            term = shares[i, :, h : h + 1] * parts[i, h].astype(F32)
            acc = term if acc is None else acc + term
        sums[pl.ds(h, rows, stride=heads), :] = acc
    out[...] = sums[...].reshape(out.shape).astype(BF16)


def merge(parts, rows, heads):
    n, width = parts.shape[0], parts.shape[-1]
    return pl.pallas_call(
        functools.partial(merge_kernel, rows, heads),
        out_shape=jax.ShapeDtypeStruct((rows, heads, width), BF16),
        in_specs=[pl.BlockSpec(memory_space=pltpu.VMEM)],
        out_specs=pl.BlockSpec(memory_space=pltpu.VMEM),
        scratch_shapes=[
            pltpu.VMEM((n, rows, width), F32),
            pltpu.VMEM((rows * heads, width), F32),
        ],
        name="merge",
    )(parts)


def block_kernel(first, tables, n_cand, has_prior, scale, valid, query, key, value, *rest):
    cands = rest[:n_cand]
    out = rest[n_cand + (1 if has_prior else 0)]
    qb, kb, vb, ab, ob, qs, ks, vs, aks, avs, os_, sems = rest[n_cand + (1 if has_prior else 0) + 1 :]
    block, group, width = qb.shape
    me = lax.axis_index("hst")
    heads = pl.ds(first, group)
    loads = [
        pltpu.make_async_copy(query.at[:, heads, :], qb, sems.at[0]),
        pltpu.make_async_copy(key.at[:, heads, :], kb, sems.at[1]),
        pltpu.make_async_copy(value.at[:, heads, :], vb, sems.at[2]),
    ]
    for load in loads:
        load.start()
    for which in range(2):
        own = (key, value)[which]

        @pl.when(me == 0)
        def _():
            pltpu.make_async_copy(
                own.at[pl.ds(0, ANCHOR), heads, :], ab.at[which], sems.at[3 + which]
            ).start()

        for index, devices in tables[which]:
            hit = functools.reduce(jnp.logical_or, [me == d for d in devices])

            @pl.when(hit)
            def _():
                pltpu.make_async_copy(cands[index], ab.at[which], sems.at[3 + which]).start()

    loads[0].wait()
    qs[...] = qb[...].astype(F32).reshape(block * group, width)
    loads[1].wait()
    ks[...] = kb[...].astype(F32).reshape(block * group, width)
    loads[2].wait()
    vs[...] = vb[...].astype(F32).reshape(block * group, width)
    for which, dst in ((0, aks), (1, avs)):
        pltpu.make_async_copy(
            key.at[pl.ds(0, ANCHOR), heads, :], ab.at[which], sems.at[3 + which]
        ).wait()
        dst[...] = ab[which].astype(F32).reshape(ANCHOR * group, width)

    row = lax.broadcasted_iota(jnp.int32, (block, block), 0)
    col = lax.broadcasted_iota(jnp.int32, (block, block), 1)
    seen = (col <= row) & (col < valid[0])
    anchored = jnp.where(me != 0, 0.0, NEG).astype(F32)
    for h in range(group):
        q = qs[pl.ds(h, block, stride=group), :].astype(BF16)
        k = ks[pl.ds(h, block, stride=group), :].astype(BF16)
        v = vs[pl.ds(h, block, stride=group), :].astype(BF16)
        ak = aks[pl.ds(h, ANCHOR, stride=group), :].astype(BF16)
        av = avs[pl.ds(h, ANCHOR, stride=group), :].astype(BF16)
        s = jnp.where(seen, dot(q, k, ((1,), (1,))) * scale, NEG)
        a = jnp.where(me != 0, dot(q, ak, ((1,), (1,))) * scale, NEG)
        peak = jnp.maximum(jnp.max(s, axis=1, keepdims=True), jnp.max(a, axis=1, keepdims=True))
        w = jnp.exp(s - peak)
        u = jnp.exp(a - peak)
        weight = jnp.sum(w, axis=1, keepdims=True) + jnp.sum(u, axis=1, keepdims=True)
        o = dot(w.astype(BF16), v, ((1,), (0,))) + dot(u.astype(BF16), av, ((1,), (0,)))
        os_[pl.ds(h, block, stride=group), :] = o / weight
    ob[...] = os_[...].reshape(block, group, width).astype(BF16)
    save = pltpu.make_async_copy(ob, out.at[:, heads, :], sems.at[5])
    save.start()
    save.wait()


def block_part(first, tables, cands, prior, valid, query, key, value, scale):
    block, heads, width = query.shape
    operands = [valid, query, key, value, *cands]
    aliases = {}
    if prior is not None:
        aliases = {len(operands): 0}
        operands.append(prior)
    return pl.pallas_call(
        functools.partial(block_kernel, first, tables, len(cands), prior is not None, scale),
        out_shape=jax.ShapeDtypeStruct(query.shape, BF16),
        in_specs=[SMEM] + [ANY] * (len(operands) - 1),
        out_specs=ANY,
        scratch_shapes=[pltpu.VMEM((block, GROUP, width), BF16)] * 3
        + [pltpu.VMEM((2, ANCHOR, GROUP, width), BF16), pltpu.VMEM((block, GROUP, width), BF16)]
        + [pltpu.VMEM((block * GROUP, width), F32)] * 3
        + [pltpu.VMEM((ANCHOR * GROUP, width), F32)] * 2
        + [pltpu.VMEM((block * GROUP, width), F32), pltpu.SemaphoreType.DMA((6,))],
        input_output_aliases=aliases,
        name=f"block{first}",
    )(*operands)


def local(n, ctx_query, ctx_key, ctx_value, valid, tail_query, tail_position):
    block, heads, width = ctx_query.shape
    rows = tail_query.shape[0]
    scale = 1.0 / math.sqrt(width)
    groups = heads // GROUP
    me = lax.axis_index("hst")
    across = 2 if n % 2 == 0 else 1
    deep = n // across

    order = [(w, g) for g in range(groups) for w in range(2)]
    if across == 2:
        cut = len(order) // 2 + 1
        up, over = order[:cut], order[cut:]
        over = over[1:] + over[:1]
    else:
        up, over = order, []
    n_up, n_over = len(up), len(over)

    def chunk(item):
        return (ctx_key, ctx_value)[item[0]][:ANCHOR, item[1] * GROUP : (item[1] + 1) * GROUP]

    place = lambda z, y: z * across + y
    is_root, is_side = me == 0, me == 1
    z_got, y_got = [], []
    found = {item: [] for item in order}
    steps_z = n_up + deep - 2
    if n_over:
        steps_z = max(steps_z, n_over + deep - 1)
    steps_y = max(n_up + n_over, n_up + deep - 1, n_over + deep) if across == 2 else 0
    bundle = up
    seq = over + up

    far = lax.all_to_all(
        pack(n, valid, tail_position, tail_query), "hst", split_axis=0, concat_axis=0, tiled=True
    )

    for s in range(max(steps_z, steps_y)):
        z_last = z_got[s - 1] if 0 < s <= len(z_got) else None
        y_last = y_got[s - 1] if 0 < s <= len(y_got) else None
        if s < steps_z:
            pairs = []
            for z in range(deep - 1):
                if 0 <= s - z < n_up:
                    pairs.append((place(z, 0), place(z + 1, 0)))
                    found[up[s - z]].append((("z", s), place(z + 1, 0)))
                if across == 2 and 0 <= s - 1 - z < n_over:
                    pairs.append((place(z, 1), place(z + 1, 1)))
                    found[over[s - 1 - z]].append((("z", s), place(z + 1, 1)))
            pay = z_last
            if pay is None:
                pay = chunk(up[s])
            else:
                if s < n_up:
                    pay = jnp.where(is_root, chunk(up[s]), pay)
                if across == 2 and 1 <= s <= n_over:
                    pay = jnp.where(is_side, y_last, pay)
            z_new = lax.ppermute(pay, "hst", pairs)
        if s < steps_y:
            pairs = []
            if s < len(seq):
                pairs.append((place(0, 0), place(0, 1)))
                found[seq[s]].append((("y", s), place(0, 1)))
            for z in range(1, deep):
                if 0 <= s - z < n_up:
                    pairs.append((place(z, 0), place(z, 1)))
                    found[up[s - z]].append((("y", s), place(z, 1)))
                if 0 <= s - 1 - z < n_over:
                    pairs.append((place(z, 1), place(z, 0)))
                    found[over[s - 1 - z]].append((("y", s), place(z, 0)))
            if z_last is None:
                pay = chunk(seq[s])
            elif s < len(seq):
                pay = jnp.where(is_root, chunk(seq[s]), z_last)
            else:
                pay = z_last
            y_got.append(lax.ppermute(pay, "hst", pairs))
        if s < steps_z:
            z_got.append(z_new)

    parts = part(valid, far, ctx_key, ctx_value, scale)
    back = lax.all_to_all(parts, "hst", split_axis=0, concat_axis=0, tiled=True)
    tail_out = merge(back, rows, heads)

    def ready(g):
        return max(max(s for (_, s), _ in found[(w, g)]) for w in range(2))

    ctx_out = None
    for g in sorted(range(groups), key=ready):
        cands, tables = [], []
        for w in range(2):
            table = {}
            for spot, device in found[(w, g)]:
                table.setdefault(spot, []).append(device)
            entries = []
            for (axis, s), devices in table.items():
                entries.append((len(cands), devices))
                cands.append((z_got if axis == "z" else y_got)[s])
            tables.append(entries)
        ctx_out = block_part(
            g * GROUP, tables, cands, ctx_out, valid, ctx_query, ctx_key, ctx_value, scale
        )
    return (ctx_out, tail_out)


def solution(mesh):
    both = ("groups", "hst")
    wide, flat = P(both, "head", None), P(both)
    return jax.shard_map(
        functools.partial(local, mesh.shape["hst"]),
        mesh=mesh,
        in_specs=(wide, wide, wide, flat, wide, flat),
        out_specs=(wide, wide),
        check_vma=False,
    )
```

```python
import functools
import math

import jax
import jax.numpy as jnp
from jax import lax
from jax.experimental import pallas as pl
from jax.experimental.pallas import tpu as pltpu
from jax.sharding import PartitionSpec as P


ANCHOR = 128
GROUP = 8
NEG = -1e30
F32 = jnp.float32
BF16 = jnp.bfloat16
ANY = pl.BlockSpec(memory_space=pl.ANY)
SMEM = pl.BlockSpec(memory_space=pltpu.SMEM)


def dot(a, b, dims):
    return lax.dot_general(a, b, (dims, ((), ())), preferred_element_type=F32)


def pack_kernel(n, valid, position, query, out):
    rows, heads, width = query.shape
    row = lax.broadcasted_iota(jnp.int32, (rows, width), 0)
    lane = lax.broadcasted_iota(jnp.int32, (rows, width), 1)
    slab = jnp.where(lane == 2, valid[0], 0)
    for r in range(rows):
        high = lax.shift_right_logical(position[r], 6)
        low = jnp.bitwise_and(position[r], 63)
        slab = jnp.where((row == r) & (lane == 0), high, slab)
        slab = jnp.where((row == r) & (lane == 1), low, slab)
    slab = slab.astype(F32).astype(BF16)
    for i in range(n):
        out[i, :rows] = query[...]
        out[i, rows, :rows] = slab
        out[i, rows, rows:] = jnp.zeros((heads - rows, width), BF16)


def pack(n, valid, position, query):
    rows, heads, width = query.shape
    return pl.pallas_call(
        functools.partial(pack_kernel, n),
        out_shape=jax.ShapeDtypeStruct((n, rows + 1, heads, width), BF16),
        in_specs=[SMEM, SMEM, pl.BlockSpec(memory_space=pltpu.VMEM)],
        out_specs=pl.BlockSpec(memory_space=pltpu.VMEM),
        name="pack",
    )(valid, position, query)


def part_kernel(rows, scale, valid, query, meta, key, value, out, stats, qs, ks, vs, ms):
    step = pl.program_id(0)
    n = query.shape[0]
    block, group, width = key.shape
    total = n * rows
    me = lax.axis_index("hst")
    qs[...] = query[:, :rows].astype(F32).reshape(total * group, width)
    ks[...] = key[...].astype(F32).reshape(block * group, width)
    vs[...] = value[...].astype(F32).reshape(block * group, width)
    for i in range(n):
        ms[i * rows : (i + 1) * rows] = meta[i, 0].astype(F32)[:rows]
    info = ms[...]
    position = info[:, 0:1] * 64.0 + info[:, 1:2]
    row = lax.broadcasted_iota(jnp.int32, (total, 1), 0)
    ahead = (row < me * rows) & (lax.rem(row, rows) == 0)
    start = jnp.sum(jnp.where(ahead, info[:, 2:3], 0.0), axis=0, keepdims=True)
    slot = lax.broadcasted_iota(jnp.int32, (total, block), 1)
    place = slot.astype(F32) + start
    seen = (place < position) & (slot < valid[0])
    lane = lax.broadcasted_iota(jnp.int32, (total, width), 1)

    @pl.when(step == 0)
    def _():
        stats[...] = jnp.full((total, width), NEG, F32)

    known = stats[...]
    for h in range(group):
        q = qs[pl.ds(h, total, stride=group), :].astype(BF16)
        k = ks[pl.ds(h, block, stride=group), :].astype(BF16)
        v = vs[pl.ds(h, block, stride=group), :].astype(BF16)
        s = jnp.where(seen, dot(q, k, ((1,), (1,))) * scale, NEG)
        peak = jnp.max(s, axis=1, keepdims=True)
        w = jnp.where(seen, jnp.exp(s - peak), 0.0)
        weight = jnp.sum(w, axis=1, keepdims=True)
        w_high = w.astype(BF16)
        w_low = (w - w_high.astype(F32)).astype(BF16)
        o = dot(w_high, v, ((1,), (0,))) + dot(w_low, v, ((1,), (0,)))
        empty = weight == 0.0
        divisor = jnp.where(empty, 1.0, weight)
        o = (o / divisor).astype(BF16)
        lse = jnp.where(empty, NEG, peak + jnp.log(divisor))
        known = jnp.where(lane == step * group + h, lse, known)
        for i in range(n):
            out[i, step * group + h] = o[i * rows : (i + 1) * rows]
    stats[...] = known

    @pl.when(step == pl.num_programs(0) - 1)
    def _():
        at = pl.num_programs(0) * group
        left = stats[...]
        for piece in range(3):
            term = left.astype(BF16)
            left = left - term.astype(F32)
            for i in range(n):
                out[i, at + piece] = term[i * rows : (i + 1) * rows]


def part(valid, far, key, value, scale):
    n, rows, heads, width = far.shape
    rows -= 1
    block = key.shape[0]
    groups = heads // GROUP
    side = pl.BlockSpec((block, GROUP, width), lambda g: (0, g, 0))
    return pl.pallas_call(
        functools.partial(part_kernel, rows, scale),
        grid=(groups,),
        out_shape=jax.ShapeDtypeStruct((n, heads + 3, rows, width), BF16),
        in_specs=[
            SMEM,
            pl.BlockSpec((n, rows + 1, GROUP, width), lambda g: (0, 0, g, 0)),
            pl.BlockSpec((n, 1, GROUP, width), lambda g: (0, rows, 0, 0)),
            side,
            side,
        ],
        out_specs=pl.BlockSpec((n, heads + 3, rows, width), lambda g: (0, 0, 0, 0)),
        scratch_shapes=[
            pltpu.VMEM((n * rows, width), F32),
            pltpu.VMEM((n * rows * GROUP, width), F32),
            pltpu.VMEM((block * GROUP, width), F32),
            pltpu.VMEM((block * GROUP, width), F32),
            pltpu.VMEM((n * rows, width), F32),
        ],
        name="part",
    )(valid, far, far, key, value)


def merge_kernel(rows, heads, parts, out, shares, sums):
    n = parts.shape[0]
    lses = []
    for i in range(n):
        pieces = [parts[i, heads + p].astype(F32) for p in range(3)]
        lses.append(pieces[0] + pieces[1] + pieces[2])
    peak = functools.reduce(jnp.maximum, lses)
    weights = [jnp.exp(lse - peak) for lse in lses]
    total = functools.reduce(jnp.add, weights)
    for i in range(n):
        shares[i] = weights[i] / total
    for h in range(heads):
        acc = None
        for i in range(n):
            term = shares[i, :, h : h + 1] * parts[i, h].astype(F32)
            acc = term if acc is None else acc + term
        sums[pl.ds(h, rows, stride=heads), :] = acc
    out[...] = sums[...].reshape(out.shape).astype(BF16)


def merge(parts, rows, heads):
    n, width = parts.shape[0], parts.shape[-1]
    return pl.pallas_call(
        functools.partial(merge_kernel, rows, heads),
        out_shape=jax.ShapeDtypeStruct((rows, heads, width), BF16),
        in_specs=[pl.BlockSpec(memory_space=pltpu.VMEM)],
        out_specs=pl.BlockSpec(memory_space=pltpu.VMEM),
        scratch_shapes=[
            pltpu.VMEM((n, rows, width), F32),
            pltpu.VMEM((rows * heads, width), F32),
        ],
        name="merge",
    )(parts)


def chunk_kernel(items, key, value, *rest):
    outs, sems = rest[:-1], rest[-1]

    @pl.when(lax.axis_index("hst") == 0)
    def _():
        copies = [
            pltpu.make_async_copy(
                (key, value)[which].at[pl.ds(0, ANCHOR), pl.ds(g * GROUP, GROUP), :],
                outs[i],
                sems.at[i],
            )
            for i, (which, g) in enumerate(items)
        ]
        for copy in copies:
            copy.start()
        for copy in copies:
            copy.wait()


def chunks_of(items, key, value):
    shape = jax.ShapeDtypeStruct((ANCHOR, GROUP, key.shape[-1]), BF16)
    outs = pl.pallas_call(
        functools.partial(chunk_kernel, items),
        out_shape=[shape] * len(items),
        in_specs=[ANY, ANY],
        out_specs=[pl.BlockSpec(memory_space=pltpu.VMEM)] * len(items),
        scratch_shapes=[pltpu.SemaphoreType.DMA((len(items),))],
        name="chunks",
    )(key, value)
    return dict(zip(items, outs))


def block_kernel(first, tables, n_cand, has_prior, scale, valid, query, key, value, *rest):
    cands = rest[:n_cand]
    out = rest[n_cand + (1 if has_prior else 0)]
    qb, kb, vb, ab, ob, qs, ks, vs, aks, avs, os_, sems = rest[n_cand + (1 if has_prior else 0) + 1 :]
    block, group, width = qb.shape
    me = lax.axis_index("hst")
    heads = pl.ds(first, group)
    loads = [
        pltpu.make_async_copy(query.at[:, heads, :], qb, sems.at[0]),
        pltpu.make_async_copy(key.at[:, heads, :], kb, sems.at[1]),
        pltpu.make_async_copy(value.at[:, heads, :], vb, sems.at[2]),
    ]
    for load in loads:
        load.start()
    for which in range(2):
        own = (key, value)[which]

        @pl.when(me == 0)
        def _():
            pltpu.make_async_copy(
                own.at[pl.ds(0, ANCHOR), heads, :], ab.at[which], sems.at[3 + which]
            ).start()

        for index, devices in tables[which]:
            hit = functools.reduce(jnp.logical_or, [me == d for d in devices])

            @pl.when(hit)
            def _():
                pltpu.make_async_copy(cands[index], ab.at[which], sems.at[3 + which]).start()

    loads[0].wait()
    qs[...] = qb[...].astype(F32).reshape(block * group, width)
    loads[1].wait()
    ks[...] = kb[...].astype(F32).reshape(block * group, width)
    loads[2].wait()
    vs[...] = vb[...].astype(F32).reshape(block * group, width)
    for which, dst in ((0, aks), (1, avs)):
        pltpu.make_async_copy(
            key.at[pl.ds(0, ANCHOR), heads, :], ab.at[which], sems.at[3 + which]
        ).wait()
        dst[...] = ab[which].astype(F32).reshape(ANCHOR * group, width)

    row = lax.broadcasted_iota(jnp.int32, (block, block), 0)
    col = lax.broadcasted_iota(jnp.int32, (block, block), 1)
    seen = (col <= row) & (col < valid[0])
    anchored = jnp.where(me != 0, 0.0, NEG).astype(F32)
    for h in range(group):
        q = qs[pl.ds(h, block, stride=group), :].astype(BF16)
        k = ks[pl.ds(h, block, stride=group), :].astype(BF16)
        v = vs[pl.ds(h, block, stride=group), :].astype(BF16)
        ak = aks[pl.ds(h, ANCHOR, stride=group), :].astype(BF16)
        av = avs[pl.ds(h, ANCHOR, stride=group), :].astype(BF16)
        s = jnp.where(seen, dot(q, k, ((1,), (1,))) * scale, NEG)
        a = jnp.where(me != 0, dot(q, ak, ((1,), (1,))) * scale, NEG)
        peak = jnp.maximum(jnp.max(s, axis=1, keepdims=True), jnp.max(a, axis=1, keepdims=True))
        w = jnp.exp(s - peak)
        u = jnp.exp(a - peak)
        weight = jnp.sum(w, axis=1, keepdims=True) + jnp.sum(u, axis=1, keepdims=True)
        o = dot(w.astype(BF16), v, ((1,), (0,))) + dot(u.astype(BF16), av, ((1,), (0,)))
        os_[pl.ds(h, block, stride=group), :] = o / weight
    ob[...] = os_[...].reshape(block, group, width).astype(BF16)
    save = pltpu.make_async_copy(ob, out.at[:, heads, :], sems.at[5])
    save.start()
    save.wait()


def block_part(first, tables, cands, prior, valid, query, key, value, scale):
    block, _, width = query.shape
    operands = [valid, query, key, value, *cands]
    aliases = {}
    if prior is not None:
        aliases = {len(operands): 0}
        operands.append(prior)
    return pl.pallas_call(
        functools.partial(block_kernel, first, tables, len(cands), prior is not None, scale),
        out_shape=jax.ShapeDtypeStruct(query.shape, BF16),
        in_specs=[SMEM] + [ANY] * (len(operands) - 1),
        out_specs=ANY,
        scratch_shapes=[pltpu.VMEM((block, GROUP, width), BF16)] * 3
        + [pltpu.VMEM((2, ANCHOR, GROUP, width), BF16), pltpu.VMEM((block, GROUP, width), BF16)]
        + [pltpu.VMEM((block * GROUP, width), F32)] * 3
        + [pltpu.VMEM((ANCHOR * GROUP, width), F32)] * 2
        + [pltpu.VMEM((block * GROUP, width), F32), pltpu.SemaphoreType.DMA((6,))],
        input_output_aliases=aliases,
    )(*operands)


def schedule(n, heads):
    groups = heads // GROUP
    order = [(w, g) for g in range(groups) for w in range(2)]
    across = 2 if n % 2 == 0 else 1
    deep = n // across
    if across == 2:
        cut = len(order) // 2 + 1
        up, over = order[:cut], order[cut:]
        over = over[1:] + over[:1]
    else:
        up, over = order, []
    place = lambda z, y: z * across + y
    seq = over + up
    z_pairs, y_pairs = [], []
    found = {item: [] for item in order}
    for s in range(len(seq) + deep + 1):
        pairs = []
        for z in range(deep - 1):
            if 0 <= s - z < len(up):
                pairs.append((place(z, 0), place(z + 1, 0)))
                found[up[s - z]].append((("z", s), place(z + 1, 0)))
            if across == 2 and 0 <= s - 1 - z < len(over):
                pairs.append((place(z, 1), place(z + 1, 1)))
                found[over[s - 1 - z]].append((("z", s), place(z + 1, 1)))
        if pairs:
            z_pairs.append(pairs)
        pairs = []
        if across == 2:
            if s < len(seq):
                pairs.append((place(0, 0), place(0, 1)))
                found[seq[s]].append((("y", s), place(0, 1)))
            for z in range(1, deep):
                if 0 <= s - z < len(up):
                    pairs.append((place(z, 0), place(z, 1)))
                    found[up[s - z]].append((("y", s), place(z, 1)))
                if 0 <= s - 1 - z < len(over):
                    pairs.append((place(z, 1), place(z, 0)))
                    found[over[s - 1 - z]].append((("y", s), place(z, 0)))
        if pairs:
            y_pairs.append(pairs)
    ready = {g: max(s for w in range(2) for (_, s), _ in found[(w, g)]) for g in range(groups)}
    return up, over, z_pairs, y_pairs, found, ready


def local(n, ctx_query, ctx_key, ctx_value, valid, tail_query, tail_position):
    return body(n, ctx_query, ctx_key, ctx_value, valid, tail_query, tail_position)


def body(n, ctx_query, ctx_key, ctx_value, valid, tail_query, tail_position):
    _, heads, width = ctx_query.shape
    rows = tail_query.shape[0]
    scale = 1.0 / math.sqrt(width)
    me = lax.axis_index("hst")
    up, over, z_pairs, y_pairs, found, ready = schedule(n, heads)
    seq = over + up
    is_root, is_side = me == 0, me == 1

    first = tuple(dict.fromkeys([up[0], seq[0]]))
    chunk = chunks_of(first, ctx_key, ctx_value)
    chunk.update(chunks_of(tuple(i for i in up + over if i not in first), ctx_key, ctx_value))

    z_got, y_got = [], []
    for s in range(max(len(z_pairs), len(y_pairs))):
        z_last = z_got[s - 1] if 0 < s <= len(z_got) else None
        y_last = y_got[s - 1] if 0 < s <= len(y_got) else None
        if s < len(z_pairs):
            pay = z_last
            if pay is None:
                pay = chunk[up[s]]
            else:
                if s < len(up):
                    pay = jnp.where(is_root, chunk[up[s]], pay)
                if 1 <= s <= len(over):
                    pay = jnp.where(is_side, y_last, pay)
            z_new = lax.ppermute(pay, "hst", z_pairs[s])
        if s < len(y_pairs):
            if z_last is None:
                pay = chunk[seq[s]]
            elif s < len(seq):
                pay = jnp.where(is_root, chunk[seq[s]], z_last)
            else:
                pay = z_last
            y_got.append(lax.ppermute(pay, "hst", y_pairs[s]))
        if s < len(z_pairs):
            z_got.append(z_new)

    message = pack(n, valid, tail_position, tail_query)
    far = lax.all_to_all(message, "hst", split_axis=0, concat_axis=0, tiled=True)
    parts = part(valid, far, ctx_key, ctx_value, scale)
    back = lax.all_to_all(parts, "hst", split_axis=0, concat_axis=0, tiled=True)
    tail_out = merge(back, rows, heads)

    ctx_out = None
    for g in sorted(ready, key=ready.get):
        cands, tables = [], []
        for w in range(2):
            table = {}
            for spot, device in found[(w, g)]:
                table.setdefault(spot, []).append(device)
            entries = []
            for (axis, s), devices in table.items():
                entries.append((len(cands), devices))
                cands.append((z_got if axis == "z" else y_got)[s])
            tables.append(entries)
        ctx_out = block_part(
            g * GROUP, tables, cands, ctx_out, valid, ctx_query, ctx_key, ctx_value, scale
        )
    return (ctx_out, tail_out)


def solution(mesh):
    both = ("groups", "hst")
    wide, flat = P(both, "head", None), P(both)
    n = mesh.shape["hst"]
    return jax.shard_map(
        functools.partial(local, n),
        mesh=mesh,
        in_specs=(wide, wide, wide, flat, wide, flat),
        out_specs=(wide, wide),
        check_vma=False,
    )
```

```python
import functools
import math

import jax
import jax.numpy as jnp
from jax import lax
from jax.experimental import pallas as pl
from jax.experimental.pallas import tpu as pltpu
from jax.sharding import PartitionSpec as P


ANCHOR = 128
GROUP = 8
PAIR = 4
NEG = -1e30
F32 = jnp.float32
BF16 = jnp.bfloat16
ANY = pl.BlockSpec(memory_space=pl.ANY)
SMEM = pl.BlockSpec(memory_space=pltpu.SMEM)


def dot(a, b, dims):
    return lax.dot_general(a, b, (dims, ((), ())), preferred_element_type=F32)


def pack_kernel(n, valid, position, query, out):
    rows, heads, width = query.shape
    row = lax.broadcasted_iota(jnp.int32, (rows, width), 0)
    lane = lax.broadcasted_iota(jnp.int32, (rows, width), 1)
    slab = jnp.where(lane == 2, valid[0], 0)
    for r in range(rows):
        high = lax.shift_right_logical(position[r], 6)
        low = jnp.bitwise_and(position[r], 63)
        slab = jnp.where((row == r) & (lane == 0), high, slab)
        slab = jnp.where((row == r) & (lane == 1), low, slab)
    slab = slab.astype(F32).astype(BF16)
    for i in range(n):
        out[i, :rows] = query[...]
        out[i, rows, :rows] = slab
        out[i, rows, rows:] = jnp.zeros((heads - rows, width), BF16)


def pack(n, valid, position, query):
    rows, heads, width = query.shape
    return pl.pallas_call(
        functools.partial(pack_kernel, n),
        out_shape=jax.ShapeDtypeStruct((n, rows + 1, heads, width), BF16),
        in_specs=[SMEM, SMEM, pl.BlockSpec(memory_space=pltpu.VMEM)],
        out_specs=pl.BlockSpec(memory_space=pltpu.VMEM),
        name="pack",
    )(valid, position, query)


def part_kernel(rows, scale, valid, query, meta, key, value, out, stats, qs, ks, vs, ms):
    step = pl.program_id(0)
    n = query.shape[0]
    block, group, width = key.shape
    total = n * rows
    me = lax.axis_index("hst")
    qs[...] = query[:, :rows].astype(F32).reshape(total * group, width)
    ks[...] = key[...].astype(F32).reshape(block * group, width)
    vs[...] = value[...].astype(F32).reshape(block * group, width)
    for i in range(n):
        ms[i * rows : (i + 1) * rows] = meta[i, 0].astype(F32)[:rows]
    info = ms[...]
    position = info[:, 0:1] * 64.0 + info[:, 1:2]
    row = lax.broadcasted_iota(jnp.int32, (total, 1), 0)
    ahead = (row < me * rows) & (lax.rem(row, rows) == 0)
    start = jnp.sum(jnp.where(ahead, info[:, 2:3], 0.0), axis=0, keepdims=True)
    slot = lax.broadcasted_iota(jnp.int32, (total, block), 1)
    place = slot.astype(F32) + start
    seen = (place < position) & (slot < valid[0])
    lane = lax.broadcasted_iota(jnp.int32, (total, width), 1)

    @pl.when(step == 0)
    def _():
        stats[...] = jnp.full((total, width), NEG, F32)

    known = stats[...]
    each = range(group)
    q = [qs[pl.ds(h, total, stride=group), :].astype(BF16) for h in each]
    k = [ks[pl.ds(h, block, stride=group), :].astype(BF16) for h in each]
    v = [vs[pl.ds(h, block, stride=group), :].astype(BF16) for h in each]
    s = [jnp.where(seen, dot(q[h], k[h], ((1,), (1,))) * scale, NEG) for h in each]
    peak = [jnp.max(s[h], axis=1, keepdims=True) for h in each]
    w = [jnp.where(seen, jnp.exp(s[h] - peak[h]), 0.0) for h in each]
    weight = [jnp.sum(w[h], axis=1, keepdims=True) for h in each]
    high = [w[h].astype(BF16) for h in each]
    low = [(w[h] - high[h].astype(F32)).astype(BF16) for h in each]
    o = [dot(high[h], v[h], ((1,), (0,))) + dot(low[h], v[h], ((1,), (0,))) for h in each]
    for h in each:
        empty = weight[h] == 0.0
        divisor = jnp.where(empty, 1.0, weight[h])
        lse = jnp.where(empty, NEG, peak[h] + jnp.log(divisor))
        known = jnp.where(lane == step * group + h, lse, known)
        o[h] = (o[h] / divisor).astype(BF16)
    for h in each:
        for i in range(n):
            out[i, step * group + h] = o[h][i * rows : (i + 1) * rows]
    stats[...] = known

    @pl.when(step == pl.num_programs(0) - 1)
    def _():
        at = pl.num_programs(0) * group
        left = stats[...]
        for piece in range(3):
            term = left.astype(BF16)
            left = left - term.astype(F32)
            for i in range(n):
                out[i, at + piece] = term[i * rows : (i + 1) * rows]


def part(valid, far, key, value, scale):
    n, rows, heads, width = far.shape
    rows -= 1
    block = key.shape[0]
    groups = heads // GROUP
    side = pl.BlockSpec((block, GROUP, width), lambda g: (0, g, 0))
    return pl.pallas_call(
        functools.partial(part_kernel, rows, scale),
        grid=(groups,),
        out_shape=jax.ShapeDtypeStruct((n, heads + 3, rows, width), BF16),
        in_specs=[
            SMEM,
            pl.BlockSpec((n, rows + 1, GROUP, width), lambda g: (0, 0, g, 0)),
            pl.BlockSpec((n, 1, GROUP, width), lambda g: (0, rows, 0, 0)),
            side,
            side,
        ],
        out_specs=pl.BlockSpec((n, heads + 3, rows, width), lambda g: (0, 0, 0, 0)),
        scratch_shapes=[
            pltpu.VMEM((n * rows, width), F32),
            pltpu.VMEM((n * rows * GROUP, width), F32),
            pltpu.VMEM((block * GROUP, width), F32),
            pltpu.VMEM((block * GROUP, width), F32),
            pltpu.VMEM((n * rows, width), F32),
        ],
        name="part",
    )(valid, far, far, key, value)


def merge_kernel(rows, heads, parts, out, shares, sums):
    n = parts.shape[0]
    lses = []
    for i in range(n):
        pieces = [parts[i, heads + p].astype(F32) for p in range(3)]
        lses.append(pieces[0] + pieces[1] + pieces[2])
    peak = functools.reduce(jnp.maximum, lses)
    weights = [jnp.exp(lse - peak) for lse in lses]
    total = functools.reduce(jnp.add, weights)
    for i in range(n):
        shares[i] = weights[i] / total
    for h in range(heads):
        acc = None
        for i in range(n):
            term = shares[i, :, h : h + 1] * parts[i, h].astype(F32)
            acc = term if acc is None else acc + term
        sums[pl.ds(h, rows, stride=heads), :] = acc
    out[...] = sums[...].reshape(out.shape).astype(BF16)


def merge(parts, rows, heads):
    n, width = parts.shape[0], parts.shape[-1]
    return pl.pallas_call(
        functools.partial(merge_kernel, rows, heads),
        out_shape=jax.ShapeDtypeStruct((rows, heads, width), BF16),
        in_specs=[pl.BlockSpec(memory_space=pltpu.VMEM)],
        out_specs=pl.BlockSpec(memory_space=pltpu.VMEM),
        scratch_shapes=[
            pltpu.VMEM((n, rows, width), F32),
            pltpu.VMEM((rows * heads, width), F32),
        ],
        name="merge",
    )(parts)


def chunk_kernel(items, key, value, *rest):
    outs, sems = rest[:-1], rest[-1]

    @pl.when(lax.axis_index("hst") == 0)
    def _():
        copies = [
            pltpu.make_async_copy(
                (key, value)[which].at[pl.ds(0, ANCHOR), pl.ds(g * GROUP, GROUP), :],
                outs[i],
                sems.at[i],
            )
            for i, (which, g) in enumerate(items)
        ]
        for copy in copies:
            copy.start()
        for copy in copies:
            copy.wait()


def chunks_of(items, key, value):
    shape = jax.ShapeDtypeStruct((ANCHOR, GROUP, key.shape[-1]), BF16)
    outs = pl.pallas_call(
        functools.partial(chunk_kernel, items),
        out_shape=[shape] * len(items),
        in_specs=[ANY, ANY],
        out_specs=[pl.BlockSpec(memory_space=pltpu.VMEM)] * len(items),
        scratch_shapes=[pltpu.SemaphoreType.DMA((len(items),))],
        name="chunks",
    )(key, value)
    return dict(zip(items, outs))


def block_kernel(first, tables, n_cand, has_prior, scale, valid, query, key, value, *rest):
    cands = rest[:n_cand]
    out = rest[n_cand + (1 if has_prior else 0)]
    qb, kb, vb, ab, ob, qs, ks, vs, aks, avs, os_, sems = rest[n_cand + (1 if has_prior else 0) + 1 :]
    block, group, width = qb.shape
    me = lax.axis_index("hst")
    heads = pl.ds(first, group)
    loads = [
        pltpu.make_async_copy(query.at[:, heads, :], qb, sems.at[0]),
        pltpu.make_async_copy(key.at[:, heads, :], kb, sems.at[1]),
        pltpu.make_async_copy(value.at[:, heads, :], vb, sems.at[2]),
    ]
    for load in loads:
        load.start()
    for which in range(2):
        own = (key, value)[which]

        @pl.when(me == 0)
        def _():
            pltpu.make_async_copy(
                own.at[pl.ds(0, ANCHOR), heads, :], ab.at[which], sems.at[3 + which]
            ).start()

        for index, devices in tables[which]:
            hit = functools.reduce(jnp.logical_or, [me == d for d in devices])

            @pl.when(hit)
            def _():
                pltpu.make_async_copy(cands[index], ab.at[which], sems.at[3 + which]).start()

    loads[0].wait()
    qs[...] = qb[...].astype(F32).reshape(block * group, width)
    loads[1].wait()
    ks[...] = kb[...].astype(F32).reshape(block * group, width)
    loads[2].wait()
    vs[...] = vb[...].astype(F32).reshape(block * group, width)
    for which, dst in ((0, aks), (1, avs)):
        pltpu.make_async_copy(
            key.at[pl.ds(0, ANCHOR), heads, :], ab.at[which], sems.at[3 + which]
        ).wait()
        dst[...] = ab[which].astype(F32).reshape(ANCHOR * group, width)

    row = lax.broadcasted_iota(jnp.int32, (block, block), 0)
    col = lax.broadcasted_iota(jnp.int32, (block, block), 1)
    seen = (col <= row) & (col < valid[0])
    anchored = jnp.where(me != 0, 0.0, NEG).astype(F32)
    for base in range(0, group, PAIR):
        each = range(base, base + PAIR)
        take = lambda ref, size: [ref[pl.ds(h, size, stride=group), :].astype(BF16) for h in each]
        q, k, v = take(qs, block), take(ks, block), take(vs, block)
        ak, av = take(aks, ANCHOR), take(avs, ANCHOR)
        each = range(PAIR)
        s = [jnp.where(seen, dot(q[h], k[h], ((1,), (1,))) * scale, NEG) for h in each]
        a = [jnp.where(me != 0, dot(q[h], ak[h], ((1,), (1,))) * scale, NEG) for h in each]
        peak = [
            jnp.maximum(jnp.max(s[h], 1, keepdims=True), jnp.max(a[h], 1, keepdims=True))
            for h in each
        ]
        w = [jnp.exp(s[h] - peak[h]) for h in each]
        u = [jnp.exp(a[h] - peak[h]) for h in each]
        weight = [jnp.sum(w[h], 1, keepdims=True) + jnp.sum(u[h], 1, keepdims=True) for h in each]
        o = [
            dot(w[h].astype(BF16), v[h], ((1,), (0,))) + dot(u[h].astype(BF16), av[h], ((1,), (0,)))
            for h in each
        ]
        for h in each:
            os_[pl.ds(base + h, block, stride=group), :] = o[h] / weight[h]
    ob[...] = os_[...].reshape(block, group, width).astype(BF16)
    save = pltpu.make_async_copy(ob, out.at[:, heads, :], sems.at[5])
    save.start()
    save.wait()


def block_part(first, tables, cands, prior, valid, query, key, value, scale):
    block, _, width = query.shape
    operands = [valid, query, key, value, *cands]
    aliases = {}
    if prior is not None:
        aliases = {len(operands): 0}
        operands.append(prior)
    return pl.pallas_call(
        functools.partial(block_kernel, first, tables, len(cands), prior is not None, scale),
        out_shape=jax.ShapeDtypeStruct(query.shape, BF16),
        in_specs=[SMEM] + [ANY] * (len(operands) - 1),
        out_specs=ANY,
        scratch_shapes=[pltpu.VMEM((block, GROUP, width), BF16)] * 3
        + [pltpu.VMEM((2, ANCHOR, GROUP, width), BF16), pltpu.VMEM((block, GROUP, width), BF16)]
        + [pltpu.VMEM((block * GROUP, width), F32)] * 3
        + [pltpu.VMEM((ANCHOR * GROUP, width), F32)] * 2
        + [pltpu.VMEM((block * GROUP, width), F32), pltpu.SemaphoreType.DMA((6,))],
        input_output_aliases=aliases,
    )(*operands)


def schedule(n, heads):
    groups = heads // GROUP
    order = [(w, g) for g in range(groups) for w in range(2)]
    across = 2 if n % 2 == 0 else 1
    deep = n // across
    if across == 2:
        cut = len(order) // 2 + 1
        up, over = order[:cut], order[cut:]
        over = over[1:] + over[:1]
    else:
        up, over = order, []
    place = lambda z, y: z * across + y
    seq = over + up
    z_pairs, y_pairs = [], []
    found = {item: [] for item in order}
    for s in range(len(seq) + deep + 1):
        pairs = []
        for z in range(deep - 1):
            if 0 <= s - z < len(up):
                pairs.append((place(z, 0), place(z + 1, 0)))
                found[up[s - z]].append((("z", s), place(z + 1, 0)))
            if across == 2 and 0 <= s - 1 - z < len(over):
                pairs.append((place(z, 1), place(z + 1, 1)))
                found[over[s - 1 - z]].append((("z", s), place(z + 1, 1)))
        if pairs:
            z_pairs.append(pairs)
        pairs = []
        if across == 2:
            if s < len(seq):
                pairs.append((place(0, 0), place(0, 1)))
                found[seq[s]].append((("y", s), place(0, 1)))
            for z in range(1, deep):
                if 0 <= s - z < len(up):
                    pairs.append((place(z, 0), place(z, 1)))
                    found[up[s - z]].append((("y", s), place(z, 1)))
                if 0 <= s - 1 - z < len(over):
                    pairs.append((place(z, 1), place(z, 0)))
                    found[over[s - 1 - z]].append((("y", s), place(z, 0)))
        if pairs:
            y_pairs.append(pairs)
    ready = {g: max(s for w in range(2) for (_, s), _ in found[(w, g)]) for g in range(groups)}
    return up, over, z_pairs, y_pairs, found, ready


def local(n, ctx_query, ctx_key, ctx_value, valid, tail_query, tail_position):
    return body(n, ctx_query, ctx_key, ctx_value, valid, tail_query, tail_position)


def body(n, ctx_query, ctx_key, ctx_value, valid, tail_query, tail_position):
    _, heads, width = ctx_query.shape
    rows = tail_query.shape[0]
    scale = 1.0 / math.sqrt(width)
    me = lax.axis_index("hst")
    up, over, z_pairs, y_pairs, found, ready = schedule(n, heads)
    seq = over + up
    is_root, is_side = me == 0, me == 1

    first = tuple(dict.fromkeys([up[0], seq[0]]))
    chunk = chunks_of(first, ctx_key, ctx_value)
    chunk.update(chunks_of(tuple(i for i in up + over if i not in first), ctx_key, ctx_value))

    z_got, y_got = [], []
    for s in range(max(len(z_pairs), len(y_pairs))):
        z_last = z_got[s - 1] if 0 < s <= len(z_got) else None
        y_last = y_got[s - 1] if 0 < s <= len(y_got) else None
        if s < len(z_pairs):
            pay = z_last
            if pay is None:
                pay = chunk[up[s]]
            else:
                if s < len(up):
                    pay = jnp.where(is_root, chunk[up[s]], pay)
                if 1 <= s <= len(over):
                    pay = jnp.where(is_side, y_last, pay)
            z_new = lax.ppermute(pay, "hst", z_pairs[s])
        if s < len(y_pairs):
            if z_last is None:
                pay = chunk[seq[s]]
            elif s < len(seq):
                pay = jnp.where(is_root, chunk[seq[s]], z_last)
            else:
                pay = z_last
            y_got.append(lax.ppermute(pay, "hst", y_pairs[s]))
        if s < len(z_pairs):
            z_got.append(z_new)

    message = pack(n, valid, tail_position, tail_query)
    far = lax.all_to_all(message, "hst", split_axis=0, concat_axis=0, tiled=True)
    parts = part(valid, far, ctx_key, ctx_value, scale)
    back = lax.all_to_all(parts, "hst", split_axis=0, concat_axis=0, tiled=True)
    tail_out = merge(back, rows, heads)

    ctx_out = None
    for g in sorted(ready, key=ready.get):
        cands, tables = [], []
        for w in range(2):
            table = {}
            for spot, device in found[(w, g)]:
                table.setdefault(spot, []).append(device)
            entries = []
            for (axis, s), devices in table.items():
                entries.append((len(cands), devices))
                cands.append((z_got if axis == "z" else y_got)[s])
            tables.append(entries)
        ctx_out = block_part(
            g * GROUP, tables, cands, ctx_out, valid, ctx_query, ctx_key, ctx_value, scale
        )
    return (ctx_out, tail_out)


def solution(mesh):
    both = ("groups", "hst")
    wide, flat = P(both, "head", None), P(both)
    n = mesh.shape["hst"]
    return jax.shard_map(
        functools.partial(local, n),
        mesh=mesh,
        in_specs=(wide, wide, wide, flat, wide, flat),
        out_specs=(wide, wide),
        check_vma=False,
    )
```
